32 devices in a mesh: seq: 8 (over y, x, core), head: 4 (over z).
Axes of the slice: x: 2, y: 2, z: 4, core: 2. Of those that a mesh axis runs over, the one named last changes fastest.
Arguments:
- values: bfloat16 [16384, 5120], P('seq', 'head'), may hold values from -6 to 6
- gates: bfloat16 [16384, 5120], P('seq', 'head'), may hold values from -6 to 6
- b_proj: bfloat16 [16384, 128], P('seq'), may hold values from -2 to 2
- c_proj: bfloat16 [16384, 128], P('seq'), may hold values from -2 to 2
- step_size: float32 [80, 16384], P('head', 'seq'), may hold values from 0.006 to 0.06
- decay_rate: float32 [80, 16384], P('head', 'seq'), may hold values from 0 to 1.2, as said below
- skip_gain: float32 [80], P('head'), may hold values from 0.5 to 2
- norm_gain: float32 [5120], P('head'), may hold values from 0.25 to 1.75
- readout_matrix: bfloat16 [5120, 2560], P('head'), may hold values from -0.078125 to 0.078125
- span_counts: int32 [8], P('seq'), may hold values from 1 to 8, as said below
- remaining_count: int32 [8], P('seq'), may hold values from 1 to 256
Outputs:
- mixer_response: bfloat16 [16384, 2560], P(('seq', 'head'))
The draws below stay inside these ranges and needn't reach their ends.
Inputs may be any that keep to these rules, and one draw needn't show every extreme that they name: `span_counts`: some shard uses all 8 span slots in every draw. `decay_rate`: Positive.
All inputs are finite; a program needn't handle non-finite values.
Results may differ from the reference program's by a relative error of at most 0.02.
Values may be sent and summed in bfloat16 or wider, within the bound.
A program may use at most 192 MiB of HBM per device.

```python
import math
import jax
import jax.numpy as jnp
from jax import lax

D = 2560
HEADS = 80
P_SIZE = 64
N = 128
SPAN = 256
CH_DEV = 8
TOK_DEV = 2048
SHARDS = 8
ENTRY_CAPACITY = 16384
N_HEAD = 4


def draw_decay_rate(key, part):
    keys = jax.random.split(key, 6)
    share = 0.5
    quick_heads = jax.random.uniform(keys[0], (HEADS,)) < share
    quick = jnp.exp(jax.random.uniform(keys[1], (HEADS,), jnp.float32, math.log(1.0 / 50.0), math.log(1.0 / 30.0)))
    slow = 0.2 * math.log(10.0) / ENTRY_CAPACITY * jnp.exp(jax.random.uniform(keys[2], (HEADS,), jnp.float32, -0.5, 0.5))
    base = jnp.where(quick_heads, quick, slow)
    blockwise = jnp.exp(jax.random.uniform(keys[3], (HEADS, ENTRY_CAPACITY // SPAN, 1), jnp.float32, -0.7, 0.7))
    rough = jax.random.uniform(keys[4], (HEADS, ENTRY_CAPACITY // SPAN, SPAN), jnp.float32, 0.5, 2.0)
    forgetting_factor = (base[:, None, None] * blockwise * rough).reshape(HEADS, ENTRY_CAPACITY)
    entry_indices = jax.random.randint(keys[5], (3,), 0, ENTRY_CAPACITY)
    element_cluster = jnp.zeros((ENTRY_CAPACITY,), jnp.float32).at[entry_indices].add(0.3)
    return (forgetting_factor + element_cluster[None, :]).astype(jnp.float32)


def draw_span_counts(key, part):
    first_key, second_key = jax.random.split(key)
    first = jax.random.randint(first_key, (SHARDS,), 0, CH_DEV)
    second = jax.random.randint(second_key, (SHARDS,), 0, CH_DEV)
    counts = 1 + first * second // (CH_DEV - 1)
    chosen = jax.random.randint(jax.random.fold_in(key, 7), (), 0, SHARDS)
    return counts.at[chosen].set(CH_DEV).astype(jnp.int32)


def place_ends(values, key, least, high):
    shape = values.shape
    place = [jax.random.randint(jax.random.fold_in(key, axis), (), 0, shape[axis]) for axis in range(len(shape))]
    values = values.at[tuple(place)].set(least)
    longest = shape.index(max(shape))
    place[longest] = (place[longest] + 1) % shape[longest]
    return values.at[tuple(place)].set(high)


def level_of(own_key, extent, pieces, low, high):
    loudness, own = 1.0, jax.random.fold_in(own_key, 6)
    for position, shards_of in pieces:
        heights = jnp.exp(jax.random.uniform(jax.random.fold_in(own, position), (shards_of,), jnp.float32, low / len(pieces), high / len(pieces)))
        loudness = loudness * jnp.repeat(heights, extent[position] // shards_of).reshape([-1 if axis == position else 1 for axis in range(len(extent))])
    return loudness


def gaussian(key, dims, scale, reach, pieces=(), kind=jnp.bfloat16):
    values = jax.random.normal(key, dims, jnp.float32) * scale
    if len(pieces) > 0:
        values = level_of(key, dims, pieces, -0.22, 0.18) * values
    return jnp.clip(values, min=-reach, max=reach).astype(kind)


def setup_inputs(seed: int = 0) -> dict:
    seeds = jax.random.split(jax.random.key(seed), 12)
    values = gaussian(seeds[0], (ENTRY_CAPACITY, HEADS * P_SIZE), 1.0, 6.0, ((0, 8), (1, 4)))
    gates = gaussian(seeds[1], (ENTRY_CAPACITY, HEADS * P_SIZE), 1.0, 6.0, ((0, 8), (1, 4)))
    b_proj = gaussian(seeds[2], (ENTRY_CAPACITY, N), 0.3, 2.0, ((0, 8),))
    c_proj = gaussian(seeds[3], (ENTRY_CAPACITY, N), 0.3, 2.0, ((0, 8),))
    step_size = jnp.clip(jnp.exp(math.log(0.06) - 2.3025851 * jax.random.uniform(seeds[4], (HEADS, ENTRY_CAPACITY), jnp.float32) ** level_of(seeds[4], (HEADS, ENTRY_CAPACITY), ((0, 4), (1, 8)), -0.2, 0.2)), 0.006, 0.06)
    decay_rate = draw_decay_rate(jax.random.fold_in(seeds[11], 71), 0)
    skip_gain = jnp.clip(0.5 + 1.5 * jax.random.uniform(seeds[6], (HEADS,), jnp.float32) ** level_of(seeds[6], (HEADS,), ((0, 4),), -0.2, 0.2), 0.5, 2.0)
    norm_gain = jnp.clip(1.0 + 0.15 * jax.random.normal(seeds[7], (HEADS * P_SIZE,), jnp.float32), 0.25, 1.75)
    readout_matrix = gaussian(seeds[8], (HEADS * P_SIZE, D), (HEADS * P_SIZE) ** -0.5, 0.078125, ((0, 4),))
    span_counts = draw_span_counts(jax.random.fold_in(seeds[11], 71), 0)
    remaining_count = place_ends(jax.random.randint(seeds[10], (SHARDS,), 1, SPAN + 1), jax.random.fold_in(seeds[10], 1), 1, SPAN).astype(jnp.int32)
    return {"values": values, "gates": gates, "b_proj": b_proj, "c_proj": c_proj, "step_size": step_size, "decay_rate": decay_rate, "skip_gain": skip_gain, "norm_gain": norm_gain, "readout_matrix": readout_matrix, "span_counts": span_counts, "remaining_count": remaining_count}


def reference(values, gates, b_proj, c_proj, step_size, decay_rate, skip_gain, norm_gain, readout_matrix, span_counts, remaining_count):
    f32 = jnp.float32
    bf16 = jnp.bfloat16
    valid = (span_counts - 1) * SPAN + remaining_count
    limit = jnp.repeat(valid, TOK_DEV)
    positioned_entries = jnp.arange(ENTRY_CAPACITY, dtype=jnp.int32) % TOK_DEV
    live = (positioned_entries < limit).astype(f32)
    blocks = ENTRY_CAPACITY // SPAN

    def spanned(array):
        return array.reshape((blocks, SPAN) + array.shape[1:])

    def per_head(array):
        return array.reshape(HEADS, blocks, SPAN).transpose(1, 0, 2)
    items = (spanned(values), spanned(gates), spanned(b_proj), spanned(c_proj), per_head(step_size), per_head(decay_rate), spanned(live))
    lower = jnp.arange(SPAN)[:, None] >= jnp.arange(SPAN)[None, :]
    group_width = HEADS * P_SIZE // N_HEAD

    def advance(state, item):
        x_span, z_span, b_span, c_span, dt_span, rate_span, live_span = item
        logdec = -rate_span * live_span[None, :]
        running = jnp.cumsum(logdec, axis=1)
        weight = dt_span * live_span[None, :]
        gram = jnp.einsum('in,jn->ij', c_span.astype(f32), b_span.astype(f32))
        spread = jnp.where(lower[None], running[:, :, None] - running[:, None, :], -1e+30)
        mixing = lax.optimization_barrier((gram[None] * jnp.exp(spread) * weight[:, None, :]).astype(bf16))
        heads_x = x_span.reshape(SPAN, HEADS, P_SIZE).astype(f32)
        inner = jnp.einsum('hij,jhp->ihp', mixing.astype(f32), heads_x)
        held = lax.optimization_barrier(state.astype(bf16))
        carried = jnp.einsum('in,hpn->ihp', c_span.astype(f32), held.astype(f32)) * jnp.exp(running).T[:, :, None]
        mixed = (inner + carried + skip_gain[None, :, None] * heads_x) * live_span[:, None, None]
        tail = jnp.exp(running[:, -1:] - running) * weight
        weighted = lax.optimization_barrier((heads_x * tail.T[:, :, None]).astype(bf16))
        fresh = jnp.einsum('jhp,jn->hpn', weighted.astype(f32), b_span.astype(f32))
        state = jnp.exp(running[:, -1])[:, None, None] * state + fresh
        gated = mixed.reshape(SPAN, HEADS * P_SIZE) * jax.nn.silu(z_span.astype(f32))
        meansq = lax.optimization_barrier(jnp.mean(gated * gated, axis=1, keepdims=True))
        normed = (gated * lax.rsqrt(meansq + 1e-05) * norm_gain[None, :]).astype(bf16)
        summed = jnp.zeros((SPAN, D), f32)
        for group in range(N_HEAD):
            lo_col = group * group_width
            partial_term = jnp.dot(normed[:, lo_col:lo_col + group_width], readout_matrix[lo_col:lo_col + group_width], preferred_element_type=f32).astype(bf16)
            summed = summed + lax.optimization_barrier(partial_term).astype(f32)
        return (state, summed.astype(bf16))
    start_state = jnp.zeros((HEADS, P_SIZE, N), f32)
    _, produced = lax.scan(advance, start_state, items)
    return produced.reshape(ENTRY_CAPACITY, D)
```

```python
import functools
import math

import jax
import jax.numpy as jnp
from jax import lax
from jax.experimental import pallas as pl
from jax.experimental.pallas import tpu as pltpu
from jax.sharding import PartitionSpec as P

SPAN = 256
LOG2E = math.log2(math.e)
F32 = jnp.float32
BF16 = jnp.bfloat16
HIGH = lax.Precision.HIGHEST
MESH = pl.DeviceIdType.MESH
VMEM = pltpu.VMEM
LIMIT = 60 * 1024 * 1024


def contract(a, b, da, db, precision=None):
    return lax.dot_general(
        a, b, (((da,), (db,)), ((), ())), precision=precision, preferred_element_type=F32
    )


def expander(heads, width):
    size = width // heads
    col = lax.broadcasted_iota(jnp.int32, (heads, width), 1) // size
    row = lax.broadcasted_iota(jnp.int32, (heads, width), 0)
    return jnp.where(col == row, 1.0, 0.0).astype(F32)


def halves(a):
    hi = a.astype(BF16)
    return hi, (a - hi.astype(F32)).astype(BF16)


def state_kernel(
    valid_ref, x_ref, b_ref, st_ref, dr_ref, runT_ref, q_ref, before_ref, lead_ref, pack_ref, s_ref, l_ref
):
    heads, length = st_ref.shape
    width = x_ref.shape[1]
    blocks = length // SPAN
    i0 = lax.broadcasted_iota(jnp.int32, (SPAN, SPAN), 0)
    i1 = lax.broadcasted_iota(jnp.int32, (SPAN, SPAN), 1)
    tril = jnp.where(i0 >= i1, 1.0, 0.0).astype(F32)
    spread = expander(heads, width)
    spread16 = spread.astype(BF16)
    s_ref[...] = jnp.zeros_like(s_ref)
    l_ref[...] = jnp.ones_like(l_ref)

    def step(c, carry):
        at = pl.ds(pl.multiple_of(c * SPAN, SPAN), SPAN)
        slot = c * SPAN + lax.broadcasted_iota(jnp.int32, (heads, SPAN), 1)
        live = slot < valid_ref[0]
        ld = jnp.where(live, dr_ref[:, at] * (-LOG2E), 0.0)
        run = contract(ld, tril, 1, 1, HIGH)
        runT = contract(tril, ld, 1, 1, HIGH)
        q = jnp.where(live, run - jnp.log2(st_ref[:, at]), 1e30)
        runT_ref[at, :] = runT
        q_ref[:, at] = q
        tail = jnp.exp2(run[:, SPAN - 1 :] - q)
        hi, lo = halves(tail)
        texp = contract(hi, spread16, 0, 0) + contract(lo, spread16, 0, 0)
        weighted = (x_ref[at, :].astype(F32) * texp).astype(BF16)
        fresh = contract(b_ref[at, :], weighted, 0, 0)
        dec = contract(jnp.exp2(runT[SPAN - 8 :, :]), spread, 1, 0, HIGH)[7:8, :]
        before_ref[c] = s_ref[...]
        lead_ref[c] = l_ref[...]
        s_ref[...] = dec * s_ref[...] + fresh
        l_ref[...] = l_ref[...] * dec
        return carry

    lax.fori_loop(0, blocks, step, 0)
    state = s_ref.shape[0]
    pack_ref[0:state, :] = s_ref[...].astype(BF16)
    total = jnp.broadcast_to(l_ref[0:1, :], (16, width))
    hi, mid = halves(total)
    low = (total - hi.astype(F32) - mid.astype(F32)).astype(BF16)
    row = lax.broadcasted_iota(jnp.int32, (16, width), 0)
    parts = jnp.where(row == 0, hi.astype(F32), jnp.where(row == 1, mid.astype(F32), low.astype(F32)))
    pack_ref[state:, :] = jnp.where(row < 3, parts, 0.0).astype(BF16)


def mix_kernel(
    ranks,
    x_ref,
    g_ref,
    b_ref,
    c_ref,
    runT_ref,
    q_ref,
    before_ref,
    lead_ref,
    all_ref,
    skip_ref,
    gain_ref,
    got_ref,
    ss_ref,
    out_buf,
    ss_buf,
    inc_ref,
    send_sem,
    recv_sem,
    ssend_sem,
    srecv_sem,
):
    heads, length = q_ref.shape
    width = x_ref.shape[1]
    blocks = length // SPAN
    each = blocks // ranks
    state = before_ref.shape[1]
    shards = all_ref.shape[0]
    me = lax.axis_index("head")
    place = lax.axis_index("seq")

    barrier = pltpu.get_barrier_semaphore()
    for k in range(1, ranks):
        pl.semaphore_signal(
            barrier, inc=1, device_id={"head": lax.rem(me + k, ranks)}, device_id_type=MESH
        )
    pl.semaphore_wait(barrier, ranks - 1)

    inc_ref[...] = jnp.zeros_like(inc_ref)

    def lap(k, carry):
        tail = all_ref[k, state:, :].astype(F32)
        decay = tail[0:1, :] + tail[1:2, :] + tail[2:3, :]
        new = decay * inc_ref[...] + all_ref[k, 0:state, :].astype(F32)
        inc_ref[...] = jnp.where(k < place, new, inc_ref[...])
        return carry

    lax.fori_loop(0, shards, lap, 0)

    spread16 = expander(heads, width).astype(BF16)
    i0 = lax.broadcasted_iota(jnp.int32, (SPAN, SPAN), 0)
    i1 = lax.broadcasted_iota(jnp.int32, (SPAN, SPAN), 1)
    lower = i0 >= i1
    left = lax.broadcasted_iota(jnp.int32, (SPAN, 128), 1) < (width // heads)
    ones = jnp.ones((8, 128), F32)

    def copies(dest, j, slot):
        c = dest * each + j
        at = pl.ds(pl.multiple_of(c * SPAN, SPAN), SPAN)
        big = pltpu.make_async_remote_copy(
            src_ref=out_buf.at[at, :],
            dst_ref=got_ref.at[slot, pl.ds(j * SPAN, SPAN), :],
            send_sem=send_sem.at[slot, j],
            recv_sem=recv_sem.at[slot, j],
            device_id={"head": dest},
            device_id_type=MESH,
        )
        small = pltpu.make_async_remote_copy(
            src_ref=ss_buf.at[c],
            dst_ref=ss_ref.at[slot, j],
            send_sem=ssend_sem.at[slot, j],
            recv_sem=srecv_sem.at[slot, j],
            device_id={"head": dest},
            device_id_type=MESH,
        )
        return big, small

    def local(j):
        c = me * each + j
        at = pl.ds(pl.multiple_of(c * SPAN, SPAN), SPAN)
        big = pltpu.make_async_copy(
            out_buf.at[at, :], got_ref.at[0, pl.ds(j * SPAN, SPAN), :], send_sem.at[0, j]
        )
        small = pltpu.make_async_copy(ss_buf.at[c], ss_ref.at[0, j], ssend_sem.at[0, j])
        return big, small

    def span(c):
        at = pl.ds(pl.multiple_of(c * SPAN, SPAN), SPAN)
        cb = c_ref[at, :]
        gram = jnp.where(lower, contract(cb, b_ref[at, :], 1, 1), 0.0)
        held = (before_ref[c] + lead_ref[c, 0:1, :] * inc_ref[...]).astype(BF16)
        runT = runT_ref[at, :]
        q = q_ref[:, at]
        hi, lo = halves(jnp.exp2(runT))
        acc = jnp.zeros((SPAN, 128), F32)
        for p in range(width // 128):
            cols = slice(p * 128, p * 128 + 128)
            xp = x_ref[at, cols]
            grow = contract(hi, spread16[:, cols], 1, 0) + contract(lo, spread16[:, cols], 1, 0)
            carried = contract(cb, held[:, cols], 1, 0) * grow
            sides = []
            for h in (2 * p, 2 * p + 1):
                m = (
                    gram * jnp.exp2(jnp.minimum(runT[:, h : h + 1] - q[h : h + 1, :], 0.0))
                ).astype(BF16)
                sides.append(jnp.dot(m, xp, preferred_element_type=F32))
            inner = jnp.where(left, sides[0], sides[1])
            z = g_ref[at, cols].astype(F32)
            gated = (inner + carried + skip_ref[:, cols] * xp.astype(F32)) * (
                z * (0.5 * jnp.tanh(0.5 * z) + 0.5)
            )
            acc = acc + gated * gated
            out_buf[at, cols] = (gated * gain_ref[:, cols]).astype(BF16)
        ss_buf[c] = contract(ones, acc, 1, 1, HIGH)

    if ranks == 4:
        order = [ranks - 1 - me, lax.rem(me + 2, ranks), me + 1 - 2 * lax.rem(me, 2)]
    else:
        order = [lax.rem(me + k, ranks) for k in range(1, ranks)]
    for index, dest in enumerate(order):
        slot = lax.rem(me - dest + ranks, ranks)

        def one(j, carry, dest=dest, slot=slot):
            span(dest * each + j)
            for copy in copies(dest, j, slot):
                copy.start()
            return carry

        lax.fori_loop(0, each, one, 0)

    def mine(j, carry):
        span(me * each + j)
        for copy in local(j):
            copy.start()
        return carry

    lax.fori_loop(0, each, mine, 0)
    for j in range(each):
        for copy in local(j):
            copy.wait()
        for dest in order:
            slot = lax.rem(me - dest + ranks, ranks)
            for copy in copies(dest, j, slot):
                copy.wait_send()
        for slot in range(1, ranks):
            for copy in copies(lax.rem(me + slot, ranks), j, slot):
                copy.wait_recv()


def body(
    ranks,
    shards,
    values,
    gates,
    b_proj,
    c_proj,
    step_size,
    decay_rate,
    skip_gain,
    norm_gain,
    readout,
    span_counts,
    remaining_count,
):
    length, width = values.shape
    heads = step_size.shape[0]
    state = b_proj.shape[1]
    blocks = length // SPAN
    me = lax.axis_index("head")
    place = lax.axis_index("seq")
    valid = (span_counts - 1) * SPAN + remaining_count
    sds = jax.ShapeDtypeStruct
    whole = pl.BlockSpec(memory_space=VMEM)

    rows = readout.shape[0] // shards
    own = lax.dynamic_slice_in_dim(readout, place * rows, rows, 0)
    moved = [
        lax.ppermute(own, "head", [((i + r) % ranks, i) for i in range(ranks)])
        for r in range(1, ranks)
    ]

    runT, q, before, lead, pack = pl.pallas_call(
        state_kernel,
        out_shape=(
            sds((length, heads), F32),
            sds((heads, length), F32),
            sds((blocks, state, width), F32),
            sds((blocks, 8, width), F32),
            sds((state + 16, width), BF16),
        ),
        in_specs=[pl.BlockSpec(memory_space=pltpu.SMEM)] + [whole] * 4,
        out_specs=(whole,) * 5,
        scratch_shapes=[VMEM((state, width), F32), VMEM((8, width), F32)],
        compiler_params=pltpu.CompilerParams(vmem_limit_bytes=LIMIT),
        cost_estimate=pl.CostEstimate(flops=10**10, bytes_accessed=12 * 10**6, transcendentals=0),
        name="span_states",
    )(valid, values, b_proj, step_size, decay_rate)

    everyone = lax.all_gather(pack, "seq")
    moved, everyone = lax.optimization_barrier((moved, everyone))
    mats = [readout] + [lax.all_gather(m, "seq", tiled=True) for m in moved]

    share = length // ranks
    each = blocks // ranks
    got, ss = pl.pallas_call(
        functools.partial(mix_kernel, ranks),
        out_shape=(sds((ranks, share, width), BF16), sds((ranks, each, 8, SPAN), F32)),
        in_specs=[whole] * 11,
        out_specs=(pl.BlockSpec(memory_space=pl.ANY), pl.BlockSpec(memory_space=pl.ANY)),
        scratch_shapes=[
            VMEM((length, width), BF16),
            VMEM((blocks, 8, SPAN), F32),
            VMEM((state, width), F32),
            pltpu.SemaphoreType.DMA((ranks, each)),
            pltpu.SemaphoreType.DMA((ranks, each)),
            pltpu.SemaphoreType.DMA((ranks, each)),
            pltpu.SemaphoreType.DMA((ranks, each)),
        ],
        compiler_params=pltpu.CompilerParams(
            vmem_limit_bytes=LIMIT, collective_id=0, has_side_effects=True
        ),
        cost_estimate=pl.CostEstimate(flops=10**11, bytes_accessed=20 * 10**6, transcendentals=0),
        name="mix_and_send",
    )(
        values,
        gates,
        b_proj,
        c_proj,
        runT,
        q,
        before,
        lead,
        everyone,
        jnp.repeat(skip_gain, width // heads)[None, :],
        norm_gain[None, :],
    )

    total = jnp.sum(ss[:, :, 0, :], axis=0).reshape(share) / (width * ranks)
    live = me * share + jnp.arange(share, dtype=jnp.int32) < valid[0]
    scale = jnp.where(live, lax.rsqrt(total + 1e-05), 0.0)
    out = sum(jnp.dot(got[r], mats[r], preferred_element_type=F32) for r in range(ranks))
    return (out * scale[:, None]).astype(BF16)


def solution(mesh):
    return jax.shard_map(
        functools.partial(body, mesh.shape["head"], mesh.shape["seq"]),
        mesh=mesh,
        in_specs=(
            P("seq", "head"),
            P("seq", "head"),
            P("seq", None),
            P("seq", None),
            P("head", "seq"),
            P("head", "seq"),
            P("head"),
            P("head"),
            P("head", None),
            P("seq"),
            P("seq"),
        ),
        out_specs=P(("seq", "head"), None),
        check_vma=False,
    )
```

```python
import functools
import math

import jax
import jax.numpy as jnp
from jax import lax
from jax.experimental import pallas as pl
from jax.experimental.pallas import tpu as pltpu
from jax.sharding import PartitionSpec as P


SPAN = 256
LOG2E = math.log2(math.e)
F32 = jnp.float32
BF16 = jnp.bfloat16
HIGH = lax.Precision.HIGHEST
MESH = pl.DeviceIdType.MESH
VMEM = pltpu.VMEM
LIMIT = 60 * 1024 * 1024


def contract(a, b, da, db, precision=None):
    return lax.dot_general(
        a, b, (((da,), (db,)), ((), ())), precision=precision, preferred_element_type=F32
    )


def expander(heads, width):
    size = width // heads
    col = lax.broadcasted_iota(jnp.int32, (heads, width), 1) // size
    row = lax.broadcasted_iota(jnp.int32, (heads, width), 0)
    return jnp.where(col == row, 1.0, 0.0).astype(F32)


def halves(a):
    hi = a.astype(BF16)
    return hi, (a - hi.astype(F32)).astype(BF16)


def state_kernel(
    valid_ref, x_ref, b_ref, st_ref, dr_ref, runT_ref, q_ref, before_ref, lead_ref, pack_ref, s_ref, l_ref
):
    heads, length = st_ref.shape
    width = x_ref.shape[1]
    blocks = length // SPAN
    i0 = lax.broadcasted_iota(jnp.int32, (SPAN, SPAN), 0)
    i1 = lax.broadcasted_iota(jnp.int32, (SPAN, SPAN), 1)
    tril = jnp.where(i0 >= i1, 1.0, 0.0).astype(F32)
    spread = expander(heads, width)
    spread16 = spread.astype(BF16)
    s_ref[...] = jnp.zeros_like(s_ref)
    l_ref[...] = jnp.ones_like(l_ref)

    def step(c, carry):
        at = pl.ds(pl.multiple_of(c * SPAN, SPAN), SPAN)
        slot = c * SPAN + lax.broadcasted_iota(jnp.int32, (heads, SPAN), 1)
        live = slot < valid_ref[0]
        ld = jnp.where(live, dr_ref[:, at] * (-LOG2E), 0.0)
        run = contract(ld, tril, 1, 1, HIGH)
        runT = contract(tril, ld, 1, 1, HIGH)
        q = jnp.where(live, run - jnp.log2(st_ref[:, at]), 1e30)
        runT_ref[at, :] = runT
        q_ref[:, at] = q
        tail = jnp.exp2(run[:, SPAN - 1 :] - q)
        hi, lo = halves(tail)
        texp = contract(hi, spread16, 0, 0) + contract(lo, spread16, 0, 0)
        weighted = (x_ref[at, :].astype(F32) * texp).astype(BF16)
        fresh = contract(b_ref[at, :], weighted, 0, 0)
        dec = contract(jnp.exp2(runT[SPAN - 8 :, :]), spread, 1, 0, HIGH)[7:8, :]
        before_ref[c] = s_ref[...]
        lead_ref[c] = l_ref[...]
        s_ref[...] = dec * s_ref[...] + fresh
        l_ref[...] = l_ref[...] * dec
        return carry

    lax.fori_loop(0, blocks, step, 0)
    state = s_ref.shape[0]
    pack_ref[0:state, :] = s_ref[...].astype(BF16)
    total = jnp.broadcast_to(l_ref[0:1, :], (16, width))
    hi, mid = halves(total)
    low = (total - hi.astype(F32) - mid.astype(F32)).astype(BF16)
    row = lax.broadcasted_iota(jnp.int32, (16, width), 0)
    parts = jnp.where(row == 0, hi.astype(F32), jnp.where(row == 1, mid.astype(F32), low.astype(F32)))
    pack_ref[state:, :] = jnp.where(row < 3, parts, 0.0).astype(BF16)


def mix_kernel(
    ranks,
    x_ref,
    g_ref,
    b_ref,
    c_ref,
    runT_ref,
    q_ref,
    before_ref,
    lead_ref,
    all_ref,
    skip_ref,
    gain_ref,
    got_ref,
    ss_ref,
    out_buf,
    ss_buf,
    inc_ref,
    send_sem,
    recv_sem,
    ssend_sem,
    srecv_sem,
):
    heads, length = q_ref.shape
    width = x_ref.shape[1]
    blocks = length // SPAN
    each = blocks // ranks
    state = before_ref.shape[1]
    shards = all_ref.shape[0]
    me = lax.axis_index("head")
    place = lax.axis_index("seq")

    barrier = pltpu.get_barrier_semaphore()
    for k in range(1, ranks):
        pl.semaphore_signal(
            barrier, inc=1, device_id={"head": lax.rem(me + k, ranks)}, device_id_type=MESH
        )
    pl.semaphore_wait(barrier, ranks - 1)

    inc_ref[...] = jnp.zeros_like(inc_ref)

    def lap(k, carry):
        tail = all_ref[k, state:, :].astype(F32)
        decay = tail[0:1, :] + tail[1:2, :] + tail[2:3, :]
        new = decay * inc_ref[...] + all_ref[k, 0:state, :].astype(F32)
        inc_ref[...] = jnp.where(k < place, new, inc_ref[...])
        return carry

    lax.fori_loop(0, shards, lap, 0)

    spread16 = expander(heads, width).astype(BF16)
    i0 = lax.broadcasted_iota(jnp.int32, (SPAN, SPAN), 0)
    i1 = lax.broadcasted_iota(jnp.int32, (SPAN, SPAN), 1)
    lower = i0 >= i1
    left = lax.broadcasted_iota(jnp.int32, (SPAN, 128), 1) < (width // heads)
    ones = jnp.ones((8, 128), F32)

    def copies(dest, j, slot):
        c = dest * each + j
        at = pl.ds(pl.multiple_of(c * SPAN, SPAN), SPAN)
        big = pltpu.make_async_remote_copy(
            src_ref=out_buf.at[at, :],
            dst_ref=got_ref.at[slot, pl.ds(j * SPAN, SPAN), :],
            send_sem=send_sem.at[slot, j],
            recv_sem=recv_sem.at[slot, j],
            device_id={"head": dest},
            device_id_type=MESH,
        )
        small = pltpu.make_async_remote_copy(
            src_ref=ss_buf.at[c],
            dst_ref=ss_ref.at[slot, j],
            send_sem=ssend_sem.at[slot, j],
            recv_sem=srecv_sem.at[slot, j],
            device_id={"head": dest},
            device_id_type=MESH,
        )
        return big, small

    def local(j):
        c = me * each + j
        at = pl.ds(pl.multiple_of(c * SPAN, SPAN), SPAN)
        big = pltpu.make_async_copy(
            out_buf.at[at, :], got_ref.at[0, pl.ds(j * SPAN, SPAN), :], send_sem.at[0, j]
        )
        small = pltpu.make_async_copy(ss_buf.at[c], ss_ref.at[0, j], ssend_sem.at[0, j])
        return big, small

    def span(c):
        at = pl.ds(pl.multiple_of(c * SPAN, SPAN), SPAN)
        cb = c_ref[at, :]
        gram = jnp.where(lower, contract(cb, b_ref[at, :], 1, 1), 0.0)
        held = (before_ref[c] + lead_ref[c, 0:1, :] * inc_ref[...]).astype(BF16)
        runT = runT_ref[at, :]
        q = q_ref[:, at]
        hi, lo = halves(jnp.exp2(runT))
        acc = jnp.zeros((SPAN, 128), F32)
        for p in range(width // 128):
            cols = slice(p * 128, p * 128 + 128)
            xp = x_ref[at, cols]
            grow = contract(hi, spread16[:, cols], 1, 0) + contract(lo, spread16[:, cols], 1, 0)
            carried = contract(cb, held[:, cols], 1, 0) * grow
            sides = []
            for h in (2 * p, 2 * p + 1):
                m = (
                    gram * jnp.exp2(jnp.minimum(runT[:, h : h + 1] - q[h : h + 1, :], 0.0))
                ).astype(BF16)
                sides.append(jnp.dot(m, xp, preferred_element_type=F32))
            inner = jnp.where(left, sides[0], sides[1])
            z = g_ref[at, cols].astype(F32)
            gated = (inner + carried + skip_ref[:, cols] * xp.astype(F32)) * (
                z * (0.5 * jnp.tanh(0.5 * z) + 0.5)
            )
            acc = acc + gated * gated
            out_buf[at, cols] = (gated * gain_ref[:, cols]).astype(BF16)
        ss_buf[c] = contract(ones, acc, 1, 1, HIGH)

    if ranks == 4:
        order = [ranks - 1 - me, lax.rem(me + 2, ranks), me + 1 - 2 * lax.rem(me, 2)]
    else:
        order = [lax.rem(me + k, ranks) for k in range(1, ranks)]
    for dest in order:
        slot = lax.rem(me - dest + ranks, ranks)

        def one(j, carry, dest=dest, slot=slot):
            span(dest * each + j)
            for copy in copies(dest, j, slot):
                copy.start()
            return carry

        lax.fori_loop(0, each, one, 0)

    def mine(j, carry):
        span(me * each + j)
        for copy in local(j):
            copy.start()
        return carry

    lax.fori_loop(0, each, mine, 0)
    for j in range(each):
        for copy in local(j):
            copy.wait()
        for dest in order:
            slot = lax.rem(me - dest + ranks, ranks)
            for copy in copies(dest, j, slot):
                copy.wait_send()
        for slot in range(1, ranks):
            for copy in copies(lax.rem(me + slot, ranks), j, slot):
                copy.wait_recv()


def readout_kernel(got_ref, scale_ref, *refs):
    total = None
    for r, mat in enumerate(refs[:-1]):
        part = jnp.dot(got_ref[r], mat[...], preferred_element_type=F32)
        total = part if total is None else total + part
    refs[-1][...] = (total * scale_ref[...]).astype(BF16)


def body(
    ranks,
    shards,
    values,
    gates,
    b_proj,
    c_proj,
    step_size,
    decay_rate,
    skip_gain,
    norm_gain,
    readout,
    span_counts,
    remaining_count,
):
    length, width = values.shape
    heads = step_size.shape[0]
    state = b_proj.shape[1]
    blocks = length // SPAN
    me = lax.axis_index("head")
    place = lax.axis_index("seq")
    valid = (span_counts - 1) * SPAN + remaining_count
    sds = jax.ShapeDtypeStruct
    whole = pl.BlockSpec(memory_space=VMEM)

    rows = readout.shape[0] // shards
    own = lax.dynamic_slice_in_dim(readout, place * rows, rows, 0)
    moved = [
        lax.ppermute(own, "head", [((i + r) % ranks, i) for i in range(ranks)])
        for r in range(1, ranks)
    ]

    spans = pl.pallas_call(
        state_kernel,
        out_shape=(
            sds((length, heads), F32),
            sds((heads, length), F32),
            sds((blocks, state, width), F32),
            sds((blocks, 8, width), F32),
            sds((state + 16, width), BF16),
        ),
        in_specs=[pl.BlockSpec(memory_space=pltpu.SMEM)] + [whole] * 4,
        out_specs=(whole,) * 5,
        scratch_shapes=[VMEM((state, width), F32), VMEM((8, width), F32)],
        compiler_params=pltpu.CompilerParams(vmem_limit_bytes=LIMIT),
        cost_estimate=pl.CostEstimate(flops=10**10, bytes_accessed=12 * 10**6, transcendentals=0),
        name="span_states",
    )
    runT, q, before, lead, pack = spans(valid, values, b_proj, step_size, decay_rate)

    everyone = lax.all_gather(pack, "seq")
    moved, everyone = lax.optimization_barrier((moved, everyone))
    mats = [readout] + [lax.all_gather(m, "seq", tiled=True) for m in moved]

    share = length // ranks
    each = blocks // ranks
    got, ss = pl.pallas_call(
        functools.partial(mix_kernel, ranks),
        out_shape=(sds((ranks, share, width), BF16), sds((ranks, each, 8, SPAN), F32)),
        in_specs=[whole] * 11,
        out_specs=(pl.BlockSpec(memory_space=pl.ANY), pl.BlockSpec(memory_space=pl.ANY)),
        scratch_shapes=[
            VMEM((length, width), BF16),
            VMEM((blocks, 8, SPAN), F32),
            VMEM((state, width), F32),
            pltpu.SemaphoreType.DMA((ranks, each)),
            pltpu.SemaphoreType.DMA((ranks, each)),
            pltpu.SemaphoreType.DMA((ranks, each)),
            pltpu.SemaphoreType.DMA((ranks, each)),
        ],
        compiler_params=pltpu.CompilerParams(
            vmem_limit_bytes=LIMIT, collective_id=0, has_side_effects=True
        ),
        cost_estimate=pl.CostEstimate(flops=10**11, bytes_accessed=20 * 10**6, transcendentals=0),
        name="mix_and_send",
    )(
        values,
        gates,
        b_proj,
        c_proj,
        runT,
        q,
        before,
        lead,
        everyone,
        jnp.repeat(skip_gain, width // heads)[None, :],
        norm_gain[None, :],
    )

    total = jnp.sum(ss[:, :, 0, :], axis=0).reshape(share) / (width * ranks)
    live = me * share + jnp.arange(share, dtype=jnp.int32) < valid[0]
    scale = jnp.where(live, lax.rsqrt(total + 1e-05), 0.0)
    depth = readout.shape[1]
    tile = 256
    return pl.pallas_call(
        readout_kernel,
        grid=(depth // tile,),
        out_shape=sds((share, depth), BF16),
        in_specs=[
            pl.BlockSpec((ranks, share, width), lambda n: (0, 0, 0)),
            pl.BlockSpec((share, 1), lambda n: (0, 0)),
        ]
        + [pl.BlockSpec((width, tile), lambda n: (0, n))] * ranks,
        out_specs=pl.BlockSpec((share, tile), lambda n: (0, n)),
        compiler_params=pltpu.CompilerParams(vmem_limit_bytes=LIMIT),
        cost_estimate=pl.CostEstimate(
            flops=2 * share * width * ranks * depth, bytes_accessed=35 * 10**6, transcendentals=0
        ),
        name="readout",
    )(got, scale[:, None], *mats)


def solution(mesh):
    return jax.shard_map(
        functools.partial(body, mesh.shape["head"], mesh.shape["seq"]),
        mesh=mesh,
        in_specs=(
            P("seq", "head"),
            P("seq", "head"),
            P("seq", None),
            P("seq", None),
            P("head", "seq"),
            P("head", "seq"),
            P("head"),
            P("head"),
            P("head", None),
            P("seq"),
            P("seq"),
        ),
        out_specs=P(("seq", "head"), None),
        check_vma=False,
    )
```
